128 devices in a mesh: pair: 2 (over core), shard: 64 (over z, y, x).
Axes of the slice: x: 4, y: 4, z: 4, core: 2. Of those that a mesh axis runs over, the one named last changes fastest.
Arguments:
- master: float32 [3072, 4096], P('shard', 'pair'), may hold values from -1.5 to 1.5
- gradient: float32 [3072, 4096], P('shard', 'pair'), may hold values from -40 to 40
- first_moment: float32 [3072, 4096], P('shard', 'pair'), may hold values from -4 to 4
- second_moment: float32 [3072, 4096], P('shard', 'pair'), may hold values from 0.02 to 4
- max_norm: float32 [1], replicated, may hold values from 768 to 1536
- step_count: int32 [1], replicated, may hold values from 1 to 1000
Outputs:
- new_master: float32 [3072, 4096], P('shard', 'pair')
- new_first: float32 [3072, 4096], P('shard', 'pair')
- new_second: float32 [3072, 4096], P('shard', 'pair')
- compute_codes: bfloat16 [3072, 4096], P('pair')
- block_scales: bfloat16 [3072, 128], P('pair')
The draws below stay inside these ranges and needn't reach their ends.
All inputs are finite; a program needn't handle non-finite values.
Results may differ from the reference program's by a relative error of at most 0.001.
The reference program's roundings to bfloat16 on the way count: a program that leaves them out, or rounds other values in their place, can miss the bound.
Values may be sent and summed in bfloat16 or wider, within the bound.
No kernel may reach another device: no remote copies, remote signals or barrier semaphores. Data moves between devices by JAX's collectives and lax.ppermute only.
A program may use at most 192 MiB of HBM per device.

```python
import math
import jax
import jax.numpy as jnp
from jax import lax

ROWS = 3072
COLS = 4096
BLOCK = 32


def draw_gradient(key, part):
    key_heads, key_halves, key_rows, key_noise = jax.random.split(key, 4)
    head_count = (ROWS + 127) // 128
    head_index = jnp.arange(ROWS) // 128
    head_log = jax.random.uniform(key_heads, (head_count,), minval=-2.0, maxval=2.0)
    head_scale = jnp.exp(head_log)[head_index][:, None]
    half_sign = jnp.where(jax.random.bernoulli(key_halves), 1.0, -1.0)
    upper_half = jnp.arange(COLS) >= COLS // 2
    half_scale = jnp.exp(0.7 * half_sign * jnp.where(upper_half, -1.0, 1.0))[None, :]
    row_scale = jnp.exp(jax.random.uniform(key_rows, (ROWS, 1), minval=-0.7, maxval=0.7))
    noise_part = jnp.clip(jax.random.normal(key_noise, (ROWS, COLS)), -6.0, 6.0)
    values = head_scale * half_scale * row_scale * noise_part
    return jnp.clip(values, -40.0, 40.0).astype(jnp.float32)


def block_scale(key, dims, cuts, low, high):
    def one(axis_at, parts):
        heights = jax.random.uniform(jax.random.fold_in(jax.random.fold_in(key, 6), axis_at), (parts,), jnp.float32, low / len(cuts), high / len(cuts))
        return jnp.repeat(jnp.exp(heights), dims[axis_at] // parts).reshape((-1,) + (1,) * (len(dims) - axis_at - 1))

    gain = one(*cuts[0])
    for cut in cuts[1:]:
        gain = gain * one(*cut)
    return gain


def noise(rng, extent, scale, limit, pieces=(), kind=jnp.bfloat16):
    loudness = block_scale(rng, extent, pieces, -0.22, 0.18) if pieces else 1.0
    drawn = jax.random.normal(rng, extent, jnp.float32) * scale * loudness
    return jnp.minimum(jnp.maximum(drawn, -limit), limit).astype(kind)


def setup_inputs(seed: int = 0) -> dict:
    streams_of = jax.random.split(jax.random.key(seed), 7)
    return {
        "master": noise(streams_of[0], (ROWS, COLS), 0.25, 1.5, ((0, 64), (1, 2)), jnp.float32),
        "gradient": draw_gradient(jax.random.fold_in(streams_of[6], 71), 0),
        "first_moment": noise(streams_of[2], (ROWS, COLS), 0.5, 4.0, ((0, 64), (1, 2)), jnp.float32),
        "second_moment": jnp.clip(jnp.exp(math.log(4.0) - 5.2983174 * jax.random.uniform(streams_of[3], (ROWS, COLS), jnp.float32) ** block_scale(streams_of[3], (ROWS, COLS), ((0, 64), (1, 2)), -0.2, 0.2)), 0.02, 4.0),
        "max_norm": jnp.clip(jax.random.uniform(streams_of[4], (1,), jnp.float32, 768.0, 1536.0), 768.0, 1536.0),
        "step_count": jax.random.randint(streams_of[5], (1,), 1, 1001).astype(jnp.int32),
    }


beta_first = 0.9
beta_second = 0.99
learn_rate = 0.01
decay_rate = 0.1
adam_eps = 1e-06
scale_floor = 0.25

def quantize(weights):
    height, width = weights.shape
    blocked = weights.reshape(height, width // BLOCK, BLOCK)
    largest = lax.optimization_barrier(jnp.max(jnp.abs(blocked), axis=2))
    scales = jnp.maximum(largest, scale_floor).astype(jnp.bfloat16)
    divided = blocked / scales.astype(jnp.float32)[:, :, None]
    return (divided.astype(jnp.bfloat16).reshape(height, width), scales)

def adam_update(master, gradient, first_moment, second_moment, max_norm, step_count, squares):
    norm_limit = max_norm[0]
    clip_factor = norm_limit / jnp.maximum(jnp.sqrt(squares), norm_limit)
    clipped = clip_factor * gradient
    new_first = beta_first * first_moment + (1.0 - beta_first) * clipped
    new_second = beta_second * second_moment + (1.0 - beta_second) * clipped * clipped
    counted = step_count[0].astype(jnp.float32)
    first_fix = 1.0 - jnp.power(jnp.full((), beta_first, jnp.float32), counted)
    second_fix = 1.0 - jnp.power(jnp.full((), beta_second, jnp.float32), counted)
    update = new_first / first_fix / (jnp.sqrt(new_second / second_fix) + adam_eps) + decay_rate * master
    new_master = master - learn_rate * update
    return (new_master, new_first, new_second)

def reference(master, gradient, first_moment, second_moment, max_norm, step_count):
    squares = jnp.sum(gradient * gradient)
    new_master, new_first, new_second = adam_update(master, gradient, first_moment, second_moment, max_norm, step_count, squares)
    compute_codes, block_scales = quantize(new_master)
    return (new_master, new_first, new_second, compute_codes, block_scales)
```

```python
import math

import jax
import jax.numpy as jnp
import numpy as np
from jax import lax
from jax.experimental import pallas as pl
from jax.experimental.pallas import tpu as pltpu
from jax.sharding import Mesh
from jax.sharding import PartitionSpec as P


BLOCK = 32
LANES = 128
AXES = ("pair", "shard_0", "shard_1", "shard_2")
SHARD = ("shard_0", "shard_1", "shard_2")
RING = 4

beta_first = 0.9
beta_second = 0.99
learn_rate = 0.01
decay_rate = 0.1
adam_eps = 1e-06
scale_floor = 0.25
log_first = math.log(float(np.float32(beta_first)))
log_second = math.log(float(np.float32(beta_second)))


def everyone():
    for p in range(2):
        for z in range(RING):
            for y in range(RING):
                for x in range(RING):
                    yield p, z, y, x


def flat(p, z, y, x):
    return ((p * RING + z) * RING + y) * RING + x


def near_mask(p):
    return 1 if p == 0 else 3


def far_mask(p):
    return 3 if p == 0 else 1


def squares_kernel(gradient_ref, out_ref):
    rows, cols = gradient_ref.shape
    total = jnp.zeros((rows, LANES), jnp.float32)
    for at in range(0, cols, LANES):
        part = gradient_ref[:, at : at + LANES]
        total = total + part * part
    line = jnp.sum(total, axis=0, keepdims=True)
    out_ref[...] = jnp.broadcast_to(line, out_ref.shape)


def adam_kernel(
    max_norm_ref, step_ref, sums_ref, master_ref, gradient_ref, first_ref, second_ref,
    new_master_ref, new_first_ref, new_second_ref, packed_ref,
):
    rows, cols = master_ref.shape
    line = jnp.sum(sums_ref[...], axis=0, keepdims=True)
    squares = jnp.sum(line, axis=1, keepdims=True)
    norm_limit = jnp.full((1, 1), max_norm_ref[0], jnp.float32)
    clip_factor = norm_limit / jnp.maximum(jnp.sqrt(squares), norm_limit)
    clip_factor = jnp.broadcast_to(clip_factor, (8, LANES))[:1]
    counted = jnp.full((8, LANES), step_ref[0].astype(jnp.float32))
    first_fix = (1.0 / (1.0 - jnp.exp(counted * log_first)))[:1]
    second_fix = (1.0 / (1.0 - jnp.exp(counted * log_second)))[:1]

    lane = lax.broadcasted_iota(jnp.int32, (rows, LANES), 1)
    last_of_block = lane % BLOCK == BLOCK - 1
    per = LANES // BLOCK
    at_row = lax.broadcasted_iota(jnp.int32, (LANES, 2 * LANES), 0)
    at_col = lax.broadcasted_iota(jnp.int32, (LANES, 2 * LANES), 1)
    spread = at_row == (at_col // BLOCK) * BLOCK + BLOCK - 1
    gathered = at_row == (at_col % per) * BLOCK + BLOCK - 1
    picks = jnp.where(
        jnp.where(at_col < LANES, spread.astype(jnp.int32), gathered.astype(jnp.int32)) == 1, 1.0, 0.0
    ).astype(jnp.bfloat16)
    group = lane // per - (cols // LANES) * lax.axis_index("pair")

    scales = jnp.zeros((rows, LANES), jnp.float32)
    for k in range(cols // LANES):
        at = slice(k * LANES, (k + 1) * LANES)
        master = master_ref[:, at]
        clipped = clip_factor * gradient_ref[:, at]
        new_first = beta_first * first_ref[:, at] + (1.0 - beta_first) * clipped
        new_second = beta_second * second_ref[:, at] + (1.0 - beta_second) * clipped * clipped
        update = new_first * first_fix / (jnp.sqrt(new_second * second_fix) + adam_eps) + decay_rate * master
        new_master = master - learn_rate * update
        new_master_ref[:, at] = new_master
        new_first_ref[:, at] = new_first
        new_second_ref[:, at] = new_second
        largest = jnp.abs(new_master)
        for shift in (1, 2, 4, 8, 16):
            largest = jnp.maximum(largest, pltpu.roll(largest, shift, 1))
        kept = jnp.where(last_of_block, jnp.maximum(largest, scale_floor), 0.0).astype(jnp.bfloat16)
        both = jnp.dot(kept, picks, preferred_element_type=jnp.float32)
        packed_ref[:, at] = (new_master / both[:, :LANES]).astype(jnp.bfloat16)
        scales = jnp.where(group == k, both[:, LANES:], scales)
    packed_ref[:, cols:] = scales.astype(jnp.bfloat16)


def place_kernel(*refs):
    pieces, (codes_ref, scales_ref, sem) = refs[:-3], refs[-3:]
    p, z, y, x = (lax.axis_index(a) for a in AXES)
    near = 1 + 2 * p
    far = 3 - 2 * p
    wide = codes_ref.shape[-1]
    copies = []
    at = 0
    for colour in range(3):
        axes = [SHARD[(colour + i) % 3] for i in range(3)]
        for bits in range(8):
            piece = pieces[at]
            at += 1
            hop = {a: (bits >> i) & 1 for i, a in enumerate(axes)}
            for j in range(8):
                zz = z ^ (far * hop[SHARD[0]]) ^ (near * (j & 1))
                yy = y ^ (far * hop[SHARD[1]]) ^ (near * ((j >> 1) & 1))
                xx = x ^ (far * hop[SHARD[2]]) ^ (near * ((j >> 2) & 1))
                away = (zz >> 1) ^ p
                owner = zz ^ (3 * away)
                row = ((owner & 1) * (RING * RING) + yy * RING + xx) * 6 + 3 * away + colour
                copies.append(pltpu.make_async_copy(piece.at[j, :, pl.ds(0, wide)], codes_ref.at[row], sem))
                copies.append(pltpu.make_async_copy(piece.at[j, :, pl.ds(wide, LANES)], scales_ref.at[row], sem))
    for copy in copies:
        copy.start()
    for copy in copies:
        copy.wait()


def permute(value, pairs):
    return lax.ppermute(value, AXES, pairs)


def redistribute(packed):
    half = packed.shape[0] // 2
    p = lax.axis_index("pair")
    home = p == lax.axis_index("shard_0") // 2
    top, low = packed[:half], packed[half:]
    one, two = [], []
    for q, z, y, x in everyone():
        if q == z // 2:
            one.append((flat(q, z, y, x), flat(q, 3 - z, y, x)))
        else:
            one.append((flat(q, z, y, x), flat(1 - q, z, y, x)))
            two.append((flat(q, z, y, x), flat(1 - q, 3 - z, y, x)))
    got_two = permute(low, two)
    got_one = permute(jnp.where(home, low, top), one)
    same = jnp.where(home, top, got_one)
    other = jnp.where(home, got_one, got_two)
    cols = packed.shape[1] - LANES
    left = jnp.where(p == 0, same, other)[:, :cols]
    right = jnp.where(p == 0, other, same)[:, :cols]
    return jnp.concatenate([left, right, same[:, cols:] + other[:, cols:]], axis=1)


def gather_pieces(block):
    rows, width = block.shape
    blocks = [block]
    for j in range(1, 8):
        pairs = []
        for q, z, y, x in everyone():
            m = near_mask(q)
            pairs.append((flat(q, z, y, x), flat(q, z ^ (m * (j & 1)), y ^ (m * ((j >> 1) & 1)), x ^ (m * (j >> 2)))))
        blocks.append(permute(block, pairs))
    whole = jnp.stack(blocks)
    third = rows // 3

    def swap(value, axis):
        pairs = []
        for q, z, y, x in everyone():
            n = [far_mask(q) if axis == i else 0 for i in range(3)]
            pairs.append((flat(q, z, y, x), flat(q, z ^ n[0], y ^ n[1], x ^ n[2])))
        return permute(value, pairs)

    pieces = [[whole[:, third * c : third * (c + 1)]] for c in range(3)]
    for step in range(3):
        count = len(pieces[0])
        for i in range(count):
            for c in range(3):
                pieces[c].append(swap(pieces[c][i], (c + step) % 3))
    return [piece for colour in pieces for piece in colour]


def per_device(master, gradient, first_moment, second_moment, max_norm, step_count):
    rows, cols = master.shape
    devices = 2 * RING**3
    f32 = jnp.float32
    own = pl.pallas_call(squares_kernel, out_shape=jax.ShapeDtypeStruct((devices, LANES), f32))(gradient)
    sums = lax.all_to_all(own, AXES, 0, 0, tiled=True)

    vmem = pl.BlockSpec(memory_space=pltpu.VMEM)
    smem = pl.BlockSpec(memory_space=pltpu.SMEM)
    new_master, new_first, new_second, packed = pl.pallas_call(
        adam_kernel,
        in_specs=[smem, smem] + [vmem] * 5,
        out_specs=[vmem] * 4,
        out_shape=[jax.ShapeDtypeStruct((rows, cols), f32)] * 3
        + [jax.ShapeDtypeStruct((rows, cols + LANES), jnp.bfloat16)],
    )(max_norm, step_count, sums, master, gradient, first_moment, second_moment)

    pieces = gather_pieces(redistribute(packed))
    groups = rows * RING**3 // 2 // 8
    anywhere = pl.BlockSpec(memory_space=pl.ANY)
    codes, scales = pl.pallas_call(
        place_kernel,
        in_specs=[anywhere] * len(pieces),
        out_specs=[anywhere] * 2,
        out_shape=[
            jax.ShapeDtypeStruct((groups, 8, 2 * cols), jnp.bfloat16),
            jax.ShapeDtypeStruct((groups, 8, LANES), jnp.bfloat16),
        ],
        scratch_shapes=[pltpu.SemaphoreType.DMA],
    )(*pieces)
    return (
        new_master,
        new_first,
        new_second,
        codes.reshape(groups * 8, 2 * cols),
        scales.reshape(groups * 8, LANES),
    )


def solution(mesh):
    finer = Mesh(mesh.devices.reshape(2, RING, RING, RING), AXES)
    state = P(SHARD, "pair")
    return jax.shard_map(
        per_device,
        mesh=finer,
        in_specs=(state, state, state, state, P(), P()),
        out_specs=(state, state, state, P("pair", None), P("pair", None)),
        check_vma=False,
    )
```

```python
import math

import jax
import jax.numpy as jnp
import numpy as np
from jax import lax
from jax.experimental import pallas as pl
from jax.experimental.pallas import tpu as pltpu
from jax.sharding import Mesh
from jax.sharding import PartitionSpec as P


BLOCK = 32
LANES = 128
AXES = ("pair", "shard_0", "shard_1", "shard_2")
SHARD = ("shard_0", "shard_1", "shard_2")
RING = 4

beta_first = 0.9
beta_second = 0.99
learn_rate = 0.01
decay_rate = 0.1
adam_eps = 1e-06
scale_floor = 0.25
log_first = math.log(float(np.float32(beta_first)))
log_second = math.log(float(np.float32(beta_second)))


def everyone():
    for p in range(2):
        for z in range(RING):
            for y in range(RING):
                for x in range(RING):
                    yield p, z, y, x


def flat(p, z, y, x):
    return ((p * RING + z) * RING + y) * RING + x


def near_mask(p):
    return 1 if p == 0 else 3


def far_mask(p):
    return 3 if p == 0 else 1


def squares_kernel(gradient_ref, out_ref):
    rows, cols = gradient_ref.shape
    total = jnp.zeros((rows, LANES), jnp.float32)
    for at in range(0, cols, LANES):
        part = gradient_ref[:, at : at + LANES]
        total = total + part * part
    line = jnp.sum(total, axis=0, keepdims=True)
    out_ref[...] = jnp.broadcast_to(line, out_ref.shape)


def adam_kernel(
    max_norm_ref, step_ref, sums_ref, master_ref, gradient_ref, first_ref, second_ref,
    new_master_ref, new_first_ref, new_second_ref, packed_ref,
):
    rows, cols = master_ref.shape
    line = jnp.sum(sums_ref[...], axis=0, keepdims=True)
    squares = jnp.sum(line, axis=1, keepdims=True)
    norm_limit = jnp.full((1, 1), max_norm_ref[0], jnp.float32)
    clip_factor = norm_limit / jnp.maximum(jnp.sqrt(squares), norm_limit)
    clip_factor = jnp.broadcast_to(clip_factor, (8, LANES))[:1]
    counted = jnp.full((8, LANES), step_ref[0].astype(jnp.float32))
    first_fix = (1.0 / (1.0 - jnp.exp(counted * log_first)))[:1]
    second_fix = (1.0 / (1.0 - jnp.exp(counted * log_second)))[:1]

    lane = lax.broadcasted_iota(jnp.int32, (rows, LANES), 1)
    last_of_block = lane % BLOCK == BLOCK - 1
    per = LANES // BLOCK
    at_row = lax.broadcasted_iota(jnp.int32, (LANES, 2 * LANES), 0)
    at_col = lax.broadcasted_iota(jnp.int32, (LANES, 2 * LANES), 1)
    spread = at_row == (at_col // BLOCK) * BLOCK + BLOCK - 1
    gathered = at_row == (at_col % per) * BLOCK + BLOCK - 1
    picks = jnp.where(
        jnp.where(at_col < LANES, spread.astype(jnp.int32), gathered.astype(jnp.int32)) == 1, 1.0, 0.0
    ).astype(jnp.bfloat16)
    group = lane // per - (cols // LANES) * lax.axis_index("pair")

    scales = jnp.zeros((rows, LANES), jnp.float32)
    for k in range(cols // LANES):
        at = slice(k * LANES, (k + 1) * LANES)
        master = master_ref[:, at]
        clipped = clip_factor * gradient_ref[:, at]
        new_first = beta_first * first_ref[:, at] + (1.0 - beta_first) * clipped
        new_second = beta_second * second_ref[:, at] + (1.0 - beta_second) * clipped * clipped
        update = new_first * first_fix / (jnp.sqrt(new_second * second_fix) + adam_eps) + decay_rate * master
        new_master = master - learn_rate * update
        new_master_ref[:, at] = new_master
        new_first_ref[:, at] = new_first
        new_second_ref[:, at] = new_second
        largest = jnp.abs(new_master)
        for shift in (1, 2, 4, 8, 16):
            largest = jnp.maximum(largest, pltpu.roll(largest, shift, 1))
        kept = jnp.where(last_of_block, jnp.maximum(largest, scale_floor), 0.0).astype(jnp.bfloat16)
        both = jnp.dot(kept, picks, preferred_element_type=jnp.float32)
        packed_ref[:, at] = (new_master / both[:, :LANES]).astype(jnp.bfloat16)
        scales = jnp.where(group == k, both[:, LANES:], scales)
    packed_ref[:, cols:] = scales.astype(jnp.bfloat16)


def place_kernel(*refs):
    pieces, (codes_ref, scales_ref, sem) = refs[:-3], refs[-3:]
    p, z, y, x = (lax.axis_index(a) for a in AXES)
    near = 1 + 2 * p
    far = 3 - 2 * p
    wide = codes_ref.shape[-1]
    copies = []
    at = 0
    for colour in range(3):
        axes = [SHARD[(colour + i) % 3] for i in range(3)]
        for bits in range(8):
            piece = pieces[at]
            at += 1
            hop = {a: (bits >> i) & 1 for i, a in enumerate(axes)}
            for j in range(8):
                zz = z ^ (far * hop[SHARD[0]]) ^ (near * (j & 1))
                yy = y ^ (far * hop[SHARD[1]]) ^ (near * ((j >> 1) & 1))
                xx = x ^ (far * hop[SHARD[2]]) ^ (near * ((j >> 2) & 1))
                away = (zz >> 1) ^ p
                owner = zz ^ (3 * away)
                row = ((owner & 1) * (RING * RING) + yy * RING + xx) * 6 + 3 * away + colour
                copies.append(pltpu.make_async_copy(piece.at[j, :, pl.ds(0, wide)], codes_ref.at[row], sem))
                copies.append(pltpu.make_async_copy(piece.at[j, :, pl.ds(wide, LANES)], scales_ref.at[row], sem))
    for copy in copies:
        copy.start()
    for copy in copies:
        copy.wait()


def permute(value, pairs):
    return lax.ppermute(value, AXES, pairs)


def redistribute(packed):
    half = packed.shape[0] // 2
    p = lax.axis_index("pair")
    home = p == lax.axis_index("shard_0") // 2
    top, low = packed[:half], packed[half:]
    one, two = [], []
    for q, z, y, x in everyone():
        if q == z // 2:
            one.append((flat(q, z, y, x), flat(q, 3 - z, y, x)))
        else:
            one.append((flat(q, z, y, x), flat(1 - q, z, y, x)))
            two.append((flat(q, z, y, x), flat(1 - q, 3 - z, y, x)))
    got_two = permute(low, two)
    got_one = permute(jnp.where(home, low, top), one)
    same = jnp.where(home, top, got_one)
    other = jnp.where(home, got_one, got_two)
    cols = packed.shape[1] - LANES
    left = jnp.where(p == 0, same, other)[:, :cols]
    right = jnp.where(p == 0, other, same)[:, :cols]
    return jnp.concatenate([left, right, same[:, cols:] + other[:, cols:]], axis=1)


def gather_pieces(block):
    rows, width = block.shape
    blocks = [block]
    for j in range(1, 8):
        pairs = []
        for q, z, y, x in everyone():
            m = near_mask(q)
            pairs.append((flat(q, z, y, x), flat(q, z ^ (m * (j & 1)), y ^ (m * ((j >> 1) & 1)), x ^ (m * (j >> 2)))))
        blocks.append(permute(block, pairs))
    whole = jnp.stack(blocks)
    third = rows // 3

    def swap(value, axis):
        pairs = []
        for q, z, y, x in everyone():
            n = [far_mask(q) if axis == i else 0 for i in range(3)]
            pairs.append((flat(q, z, y, x), flat(q, z ^ n[0], y ^ n[1], x ^ n[2])))
        return permute(value, pairs)

    pieces = [[whole[:, third * c : third * (c + 1)]] for c in range(3)]
    for step in range(3):
        count = len(pieces[0])
        for i in range(count):
            for c in range(3):
                pieces[c].append(swap(pieces[c][i], (c + step) % 3))
    return [piece for colour in pieces for piece in colour]


def per_device(master, gradient, first_moment, second_moment, max_norm, step_count):
    rows, cols = master.shape
    devices = 2 * RING**3
    f32 = jnp.float32
    own = pl.pallas_call(squares_kernel, out_shape=jax.ShapeDtypeStruct((devices, LANES), f32),
        compiler_params=pltpu.CompilerParams(vmem_limit_bytes=4 << 20))(gradient)
    sums = lax.all_to_all(own, AXES, 0, 0, tiled=True)

    vmem = pl.BlockSpec(memory_space=pltpu.VMEM)
    smem = pl.BlockSpec(memory_space=pltpu.SMEM)
    new_master, new_first, new_second, packed = pl.pallas_call(
        adam_kernel,
        in_specs=[smem, smem] + [vmem] * 5,
        out_specs=[vmem] * 4,
        out_shape=[jax.ShapeDtypeStruct((rows, cols), f32)] * 3
        + [jax.ShapeDtypeStruct((rows, cols + LANES), jnp.bfloat16)],
        compiler_params=pltpu.CompilerParams(vmem_limit_bytes=8 << 20),
    )(max_norm, step_count, sums, master, gradient, first_moment, second_moment)

    pieces = gather_pieces(redistribute(packed))
    groups = rows * RING**3 // 2 // 8
    anywhere = pl.BlockSpec(memory_space=pl.ANY)
    codes, scales = pl.pallas_call(
        place_kernel,
        in_specs=[anywhere] * len(pieces),
        out_specs=[anywhere] * 2,
        out_shape=[
            jax.ShapeDtypeStruct((groups, 8, 2 * cols), jnp.bfloat16),
            jax.ShapeDtypeStruct((groups, 8, LANES), jnp.bfloat16),
        ],
        scratch_shapes=[pltpu.SemaphoreType.DMA],
        compiler_params=pltpu.CompilerParams(vmem_limit_bytes=1 << 20),
    )(*pieces)
    return (
        new_master,
        new_first,
        new_second,
        codes.reshape(groups * 8, 2 * cols),
        scales.reshape(groups * 8, LANES),
    )


def solution(mesh):
    finer = Mesh(mesh.devices.reshape(2, RING, RING, RING), AXES)
    state = P(SHARD, "pair")
    return jax.shard_map(
        per_device,
        mesh=finer,
        in_specs=(state, state, state, state, P(), P()),
        out_specs=(state, state, state, P("pair", None), P("pair", None)),
        check_vma=False,
    )
```

```python
import functools
import math

import jax
import jax.numpy as jnp
import numpy as np
from jax import lax
from jax.experimental import pallas as pl
from jax.experimental.pallas import tpu as pltpu
from jax.sharding import Mesh
from jax.sharding import PartitionSpec as P


BLOCK = 32
LANES = 128
AXES = ("pair", "shard_0", "shard_1", "shard_2")
SHARD = ("shard_0", "shard_1", "shard_2")
RING = 4

beta_first = 0.9
beta_second = 0.99
learn_rate = 0.01
decay_rate = 0.1
adam_eps = 1e-06
scale_floor = 0.25
log_first = math.log(float(np.float32(beta_first)))
log_second = math.log(float(np.float32(beta_second)))


def everyone():
    for p in range(2):
        for z in range(RING):
            for y in range(RING):
                for x in range(RING):
                    yield p, z, y, x


def flat(p, z, y, x):
    return ((p * RING + z) * RING + y) * RING + x


def near_mask(p):
    return 1 if p == 0 else 3


def far_mask(p):
    return 3 if p == 0 else 1


def squares_kernel(
    max_norm_ref, step_ref, master_in, gradient_in, first_in, second_in,
    sums_ref, known_ref, master_ref, gradient_ref, first_ref, second_ref, sems,
):
    copies = [
        pltpu.make_async_copy(source, target, sems.at[i])
        for i, (source, target) in enumerate(
            [(gradient_in, gradient_ref), (master_in, master_ref), (first_in, first_ref), (second_in, second_ref)]
        )
    ]
    for copy in copies:
        copy.start()
    counted = jnp.full((1, LANES), step_ref[0].astype(jnp.float32))
    known_ref[0:1, :] = jnp.full((1, LANES), max_norm_ref[0], jnp.float32)
    known_ref[1:2, :] = 1.0 / (1.0 - jnp.exp(counted * log_first))
    known_ref[2:3, :] = 1.0 / (1.0 - jnp.exp(counted * log_second))
    known_ref[3:, :] = jnp.zeros((known_ref.shape[0] - 3, LANES), jnp.float32)
    copies[0].wait()
    rows, cols = gradient_ref.shape
    total = jnp.zeros((rows, LANES), jnp.float32)
    for at in range(0, cols, LANES):
        part = gradient_ref[:, at : at + LANES]
        total = total + part * part
    line = jnp.sum(total, axis=0, keepdims=True)
    sums_ref[...] = jnp.broadcast_to(line, sums_ref.shape)
    for copy in copies[1:]:
        copy.wait()


def adam_kernel(
    sums_ref, known_ref, master_ref, gradient_ref, first_ref, second_ref,
    new_master_ref, new_first_ref, new_second_ref, top_ref, low_ref, one_ref,
):
    rows, cols = master_ref.shape
    line = jnp.sum(sums_ref[...], axis=0, keepdims=True)
    squares = jnp.sum(line, axis=1, keepdims=True)
    norm_limit = known_ref[0:1, :]
    clip_factor = norm_limit / jnp.maximum(jnp.sqrt(squares), norm_limit)
    first_fix = known_ref[1:2, :]
    second_fix = known_ref[2:3, :]

    lane = lax.broadcasted_iota(jnp.int32, (rows, LANES), 1)
    last_of_block = lane % BLOCK == BLOCK - 1
    per = LANES // BLOCK
    at_row = lax.broadcasted_iota(jnp.int32, (LANES, 2 * LANES), 0)
    at_col = lax.broadcasted_iota(jnp.int32, (LANES, 2 * LANES), 1)
    spread = at_row == (at_col // BLOCK) * BLOCK + BLOCK - 1
    gathered = at_row == (at_col % per) * BLOCK + BLOCK - 1
    picks = jnp.where(
        jnp.where(at_col < LANES, spread.astype(jnp.int32), gathered.astype(jnp.int32)) == 1, 1.0, 0.0
    ).astype(jnp.bfloat16)
    group = lane // per - (cols // LANES) * lax.axis_index("pair")

    home = lax.axis_index("pair") == lax.axis_index("shard_0") // 2

    def store(at, values):
        top, low = values[: rows // 2], values[rows // 2 :]
        top_ref[:, at] = top.astype(jnp.bfloat16)
        low_ref[:, at] = low.astype(jnp.bfloat16)
        one_ref[:, at] = jnp.where(home, low, top).astype(jnp.bfloat16)

    scales = jnp.zeros((rows, LANES), jnp.float32)
    for k in range(cols // LANES):
        at = slice(k * LANES, (k + 1) * LANES)
        master = master_ref[:, at]
        clipped = clip_factor * gradient_ref[:, at]
        new_first = beta_first * first_ref[:, at] + (1.0 - beta_first) * clipped
        new_second = beta_second * second_ref[:, at] + (1.0 - beta_second) * clipped * clipped
        update = new_first * first_fix / (jnp.sqrt(new_second * second_fix) + adam_eps) + decay_rate * master
        new_master = master - learn_rate * update
        new_master_ref[:, at] = new_master
        new_first_ref[:, at] = new_first
        new_second_ref[:, at] = new_second
        largest = jnp.abs(new_master)
        for shift in (1, 2, 4, 8, 16):
            largest = jnp.maximum(largest, pltpu.roll(largest, shift, 1))
        kept = jnp.where(last_of_block, jnp.maximum(largest, scale_floor), 0.0).astype(jnp.bfloat16)
        both = jnp.dot(kept, picks, preferred_element_type=jnp.float32)
        store(at, new_master / both[:, :LANES])
        scales = jnp.where(group == k, both[:, LANES:], scales)
    store(slice(cols, cols + LANES), scales)


def join_kernel(top_ref, one_ref, two_ref, out_ref):
    p = lax.axis_index("pair")
    home = lax.axis_index("shard_0") // 2
    cols = top_ref.shape[1] - LANES

    def fill(left, right):
        out_ref[:, :cols] = left[:, :cols]
        out_ref[:, cols : 2 * cols] = right[:, :cols]
        out_ref[:, 2 * cols :] = left[:, cols:] + right[:, cols:]

    pl.when((p == 0) & (home == 0))(lambda: fill(top_ref, one_ref))
    pl.when((p == 1) & (home == 1))(lambda: fill(one_ref, top_ref))
    pl.when((p == 0) & (home == 1))(lambda: fill(one_ref, two_ref))
    pl.when((p == 1) & (home == 0))(lambda: fill(two_ref, one_ref))


def place_kernel(which, *refs):
    pieces, (codes_ref, scales_ref, sem) = refs[: len(which)], refs[-3:]
    p, z, y, x = (lax.axis_index(a) for a in AXES)
    near = 1 + 2 * p
    far = 3 - 2 * p
    wide = codes_ref.shape[-1]
    copies = []
    for piece, (colour, bits) in zip(pieces, which):
        hop = {SHARD[(colour + i) % 3]: (bits >> i) & 1 for i in range(3)}
        for j in range(8):
            zz = z ^ (far * hop[SHARD[0]]) ^ (near * (j & 1))
            yy = y ^ (far * hop[SHARD[1]]) ^ (near * ((j >> 1) & 1))
            xx = x ^ (far * hop[SHARD[2]]) ^ (near * ((j >> 2) & 1))
            away = (zz >> 1) ^ p
            owner = zz ^ (3 * away)
            row = ((owner & 1) * (RING * RING) + yy * RING + xx) * 6 + 3 * away + colour
            copies.append(pltpu.make_async_copy(piece.at[j, :, pl.ds(0, wide)], codes_ref.at[row], sem))
            copies.append(pltpu.make_async_copy(piece.at[j, :, pl.ds(wide, LANES)], scales_ref.at[row], sem))
    for copy in copies:
        copy.start()
    for copy in copies:
        copy.wait()


def permute(value, pairs):
    return lax.ppermute(value, AXES, pairs)


def redistribute(top, low, first):
    one, two = [], []
    for q, z, y, x in everyone():
        if q == z // 2:
            one.append((flat(q, z, y, x), flat(q, 3 - z, y, x)))
        else:
            one.append((flat(q, z, y, x), flat(1 - q, z, y, x)))
            two.append((flat(q, z, y, x), flat(1 - q, 3 - z, y, x)))
    got_two = permute(low, two)
    got_one = permute(first, one)
    rows, width = top.shape
    vmem = pl.BlockSpec(memory_space=pltpu.VMEM)
    return pl.pallas_call(
        join_kernel,
        in_specs=[vmem] * 3,
        out_specs=vmem,
        out_shape=jax.ShapeDtypeStruct((rows, 2 * width - LANES), top.dtype),
        compiler_params=pltpu.CompilerParams(vmem_limit_bytes=2 << 20),
    )(top, got_one, got_two)


def gather_pieces(block):
    rows, width = block.shape
    blocks = [block]
    for j in range(1, 8):
        pairs = []
        for q, z, y, x in everyone():
            m = near_mask(q)
            pairs.append((flat(q, z, y, x), flat(q, z ^ (m * (j & 1)), y ^ (m * ((j >> 1) & 1)), x ^ (m * (j >> 2)))))
        blocks.append(permute(block, pairs))
    whole = jnp.stack(blocks)
    third = rows // 3

    def swap(value, axis):
        pairs = []
        for q, z, y, x in everyone():
            n = [far_mask(q) if axis == i else 0 for i in range(3)]
            pairs.append((flat(q, z, y, x), flat(q, z ^ n[0], y ^ n[1], x ^ n[2])))
        return permute(value, pairs)

    pieces = [[whole[:, third * c : third * (c + 1)]] for c in range(3)]
    for step in range(3):
        count = len(pieces[0])
        for i in range(count):
            for c in range(3):
                pieces[c].append(swap(pieces[c][i], (c + step) % 3))
    return pieces


def per_device(master, gradient, first_moment, second_moment, max_norm, step_count):
    rows, cols = master.shape
    devices = 2 * RING**3
    f32 = jnp.float32
    state = jax.ShapeDtypeStruct((rows, cols), f32)
    vmem = pl.BlockSpec(memory_space=pltpu.VMEM)
    smem = pl.BlockSpec(memory_space=pltpu.SMEM)
    anywhere = pl.BlockSpec(memory_space=pl.ANY)
    hbm = pl.BlockSpec(memory_space=pltpu.HBM)
    own, known, master, gradient, first_moment, second_moment = pl.pallas_call(
        squares_kernel,
        in_specs=[smem, smem] + [hbm] * 4,
        out_specs=[vmem] * 6,
        out_shape=[jax.ShapeDtypeStruct((devices, LANES), f32), jax.ShapeDtypeStruct((8, LANES), f32)] + [state] * 4,
        scratch_shapes=[pltpu.SemaphoreType.DMA((4,))],
        compiler_params=pltpu.CompilerParams(vmem_limit_bytes=4 << 20),
    )(max_norm, step_count, master, gradient, first_moment, second_moment)
    sums = lax.all_to_all(own, AXES, 0, 0, tiled=True)

    half = jax.ShapeDtypeStruct((rows // 2, cols + LANES), jnp.bfloat16)
    new_master, new_first, new_second, top, low, first = pl.pallas_call(
        adam_kernel,
        in_specs=[vmem] * 6,
        out_specs=[vmem] * 6,
        out_shape=[state] * 3 + [half] * 3,
        compiler_params=pltpu.CompilerParams(vmem_limit_bytes=8 << 20),
    )(sums, known, master, gradient, first_moment, second_moment)

    pieces = gather_pieces(redistribute(top, low, first))
    groups = rows * RING**3 // 2 // 8
    outs = ()
    for bits in ((0, 1, 2, 3), (4, 5, 6), (7,)):
        which = [(c, b) for b in bits for c in range(3)]
        outs = pl.pallas_call(
            functools.partial(place_kernel, which),
            in_specs=[anywhere] * (len(which) + len(outs)),
            out_specs=[anywhere] * 2,
            out_shape=[
                jax.ShapeDtypeStruct((groups, 8, 2 * cols), jnp.bfloat16),
                jax.ShapeDtypeStruct((groups, 8, LANES), jnp.bfloat16),
            ],
            input_output_aliases={len(which) + i: i for i in range(len(outs))},
            scratch_shapes=[pltpu.SemaphoreType.DMA],
            compiler_params=pltpu.CompilerParams(vmem_limit_bytes=1 << 20),
        )(*[pieces[c][b] for c, b in which], *outs)
    codes, scales = outs
    return (
        new_master,
        new_first,
        new_second,
        codes.reshape(groups * 8, 2 * cols),
        scales.reshape(groups * 8, LANES),
    )


def solution(mesh):
    finer = Mesh(mesh.devices.reshape(2, RING, RING, RING), AXES)
    state = P(SHARD, "pair")
    return jax.shard_map(
        per_device,
        mesh=finer,
        in_specs=(state, state, state, state, P(), P()),
        out_specs=(state, state, state, P("pair", None), P("pair", None)),
        check_vma=False,
    )
```

```python
import functools
import math

import jax
import jax.numpy as jnp
import numpy as np
from jax import lax
from jax.experimental import pallas as pl
from jax.experimental.pallas import tpu as pltpu
from jax.sharding import Mesh
from jax.sharding import PartitionSpec as P


BLOCK = 32
LANES = 128
AXES = ("pair", "shard_0", "shard_1", "shard_2")
SHARD = ("shard_0", "shard_1", "shard_2")
RING = 4

beta_first = 0.9
beta_second = 0.99
learn_rate = 0.01
decay_rate = 0.1
adam_eps = 1e-06
scale_floor = 0.25
log_first = math.log(float(np.float32(beta_first)))
log_second = math.log(float(np.float32(beta_second)))


def everyone():
    for p in range(2):
        for z in range(RING):
            for y in range(RING):
                for x in range(RING):
                    yield p, z, y, x


def flat(p, z, y, x):
    return ((p * RING + z) * RING + y) * RING + x


def near_mask(p):
    return 1 if p == 0 else 3


def far_mask(p):
    return 3 if p == 0 else 1


def squares_kernel(
    max_norm_ref, step_ref, gradient_ref, sums_ref, known_ref
):
    counted = jnp.full((1, LANES), step_ref[0].astype(jnp.float32))
    known_ref[0:1, :] = jnp.full((1, LANES), max_norm_ref[0], jnp.float32)
    known_ref[1:2, :] = 1.0 / (1.0 - jnp.exp(counted * log_first))
    known_ref[2:3, :] = 1.0 / (1.0 - jnp.exp(counted * log_second))
    known_ref[3:, :] = jnp.zeros((known_ref.shape[0] - 3, LANES), jnp.float32)
    rows, cols = gradient_ref.shape
    total = jnp.zeros((rows, LANES), jnp.float32)
    for at in range(0, cols, LANES):
        part = gradient_ref[:, at : at + LANES]
        total = total + part * part
    line = jnp.sum(total, axis=0, keepdims=True)
    sums_ref[...] = jnp.broadcast_to(line, sums_ref.shape)


def adam_kernel(
    sums_ref, known_ref, master_ref, gradient_ref, first_ref, second_ref,
    new_master_ref, new_first_ref, new_second_ref, top_ref, low_ref, one_ref,
):
    rows, cols = master_ref.shape
    line = jnp.sum(sums_ref[...], axis=0, keepdims=True)
    squares = jnp.sum(line, axis=1, keepdims=True)
    norm_limit = known_ref[0:1, :]
    clip_factor = norm_limit / jnp.maximum(jnp.sqrt(squares), norm_limit)
    first_fix = known_ref[1:2, :]
    second_fix = known_ref[2:3, :]

    lane = lax.broadcasted_iota(jnp.int32, (rows, LANES), 1)
    last_of_block = lane % BLOCK == BLOCK - 1
    per = LANES // BLOCK
    at_row = lax.broadcasted_iota(jnp.int32, (LANES, 2 * LANES), 0)
    at_col = lax.broadcasted_iota(jnp.int32, (LANES, 2 * LANES), 1)
    spread = at_row == (at_col // BLOCK) * BLOCK + BLOCK - 1
    gathered = at_row == (at_col % per) * BLOCK + BLOCK - 1
    picks = jnp.where(
        jnp.where(at_col < LANES, spread.astype(jnp.int32), gathered.astype(jnp.int32)) == 1, 1.0, 0.0
    ).astype(jnp.bfloat16)
    group = lane // per - (cols // LANES) * lax.axis_index("pair")

    home = lax.axis_index("pair") == lax.axis_index("shard_0") // 2

    def store(at, values):
        top, low = values[: rows // 2], values[rows // 2 :]
        top_ref[:, at] = top.astype(jnp.bfloat16)
        low_ref[:, at] = low.astype(jnp.bfloat16)
        one_ref[:, at] = jnp.where(home, low, top).astype(jnp.bfloat16)

    scales = jnp.zeros((rows, LANES), jnp.float32)
    for k in range(cols // LANES):
        at = slice(k * LANES, (k + 1) * LANES)
        master = master_ref[:, at]
        clipped = clip_factor * gradient_ref[:, at]
        new_first = beta_first * first_ref[:, at] + (1.0 - beta_first) * clipped
        new_second = beta_second * second_ref[:, at] + (1.0 - beta_second) * clipped * clipped
        update = new_first * first_fix / (jnp.sqrt(new_second * second_fix) + adam_eps) + decay_rate * master
        new_master = master - learn_rate * update
        new_master_ref[:, at] = new_master
        new_first_ref[:, at] = new_first
        new_second_ref[:, at] = new_second
        largest = jnp.abs(new_master)
        for shift in (1, 2, 4, 8, 16):
            largest = jnp.maximum(largest, pltpu.roll(largest, shift, 1))
        kept = jnp.where(last_of_block, jnp.maximum(largest, scale_floor), 0.0).astype(jnp.bfloat16)
        both = jnp.dot(kept, picks, preferred_element_type=jnp.float32)
        store(at, new_master / both[:, :LANES])
        scales = jnp.where(group == k, both[:, LANES:], scales)
    store(slice(cols, cols + LANES), scales)


def join_kernel(top_ref, one_ref, two_ref, out_ref):
    p = lax.axis_index("pair")
    home = lax.axis_index("shard_0") // 2
    cols = top_ref.shape[1] - LANES

    def fill(left, right):
        out_ref[:, :cols] = left[:, :cols]
        out_ref[:, cols : 2 * cols] = right[:, :cols]
        out_ref[:, 2 * cols :] = left[:, cols:] + right[:, cols:]

    pl.when((p == 0) & (home == 0))(lambda: fill(top_ref, one_ref))
    pl.when((p == 1) & (home == 1))(lambda: fill(one_ref, top_ref))
    pl.when((p == 0) & (home == 1))(lambda: fill(one_ref, two_ref))
    pl.when((p == 1) & (home == 0))(lambda: fill(two_ref, one_ref))


def place_kernel(which, *refs):
    pieces, (codes_ref, scales_ref, sem) = refs[: len(which)], refs[-3:]
    p, z, y, x = (lax.axis_index(a) for a in AXES)
    near = 1 + 2 * p
    far = 3 - 2 * p
    wide = codes_ref.shape[-1]
    copies = []
    for piece, (colour, bits) in zip(pieces, which):
        hop = {SHARD[(colour + i) % 3]: (bits >> i) & 1 for i in range(3)}
        for j in range(8):
            zz = z ^ (far * hop[SHARD[0]]) ^ (near * (j & 1))
            yy = y ^ (far * hop[SHARD[1]]) ^ (near * ((j >> 1) & 1))
            xx = x ^ (far * hop[SHARD[2]]) ^ (near * ((j >> 2) & 1))
            away = (zz >> 1) ^ p
            owner = zz ^ (3 * away)
            row = ((owner & 1) * (RING * RING) + yy * RING + xx) * 6 + 3 * away + colour
            copies.append(pltpu.make_async_copy(piece.at[j, :, pl.ds(0, wide)], codes_ref.at[row], sem))
            copies.append(pltpu.make_async_copy(piece.at[j, :, pl.ds(wide, LANES)], scales_ref.at[row], sem))
    for copy in copies:
        copy.start()
    for copy in copies:
        copy.wait()


def permute(value, pairs):
    return lax.ppermute(value, AXES, pairs)


def redistribute(top, low, first):
    one, two = [], []
    for q, z, y, x in everyone():
        if q == z // 2:
            one.append((flat(q, z, y, x), flat(q, 3 - z, y, x)))
        else:
            one.append((flat(q, z, y, x), flat(1 - q, z, y, x)))
            two.append((flat(q, z, y, x), flat(1 - q, 3 - z, y, x)))
    got_two = permute(low, two)
    got_one = permute(first, one)
    rows, width = top.shape
    vmem = pl.BlockSpec(memory_space=pltpu.VMEM)
    return pl.pallas_call(
        join_kernel,
        in_specs=[vmem] * 3,
        out_specs=vmem,
        out_shape=jax.ShapeDtypeStruct((rows, 2 * width - LANES), top.dtype),
        compiler_params=pltpu.CompilerParams(vmem_limit_bytes=2 << 20),
    )(top, got_one, got_two)


def gather_pieces(block):
    rows, _ = block.shape
    blocks = [block]
    for j in range(1, 8):
        pairs = []
        for q, z, y, x in everyone():
            m = near_mask(q)
            pairs.append((flat(q, z, y, x), flat(q, z ^ (m * (j & 1)), y ^ (m * ((j >> 1) & 1)), x ^ (m * (j >> 2)))))
        blocks.append(permute(block, pairs))
    whole = jnp.stack(blocks)
    third = rows // 3

    def swap(value, axis):
        pairs = []
        for q, z, y, x in everyone():
            n = [far_mask(q) if axis == i else 0 for i in range(3)]
            pairs.append((flat(q, z, y, x), flat(q, z ^ n[0], y ^ n[1], x ^ n[2])))
        return permute(value, pairs)

    pieces = [[whole[:, third * c : third * (c + 1)]] for c in range(3)]
    for step in range(3):
        count = len(pieces[0])
        for i in range(count):
            for c in range(3):
                pieces[c].append(swap(pieces[c][i], (c + step) % 3))
    return pieces


def per_device(master, gradient, first_moment, second_moment, max_norm, step_count):
    rows, cols = master.shape
    devices = 2 * RING**3
    f32 = jnp.float32
    state = jax.ShapeDtypeStruct((rows, cols), f32)
    vmem = pl.BlockSpec(memory_space=pltpu.VMEM)
    smem = pl.BlockSpec(memory_space=pltpu.SMEM)
    anywhere = pl.BlockSpec(memory_space=pl.ANY)
    own, known = pl.pallas_call(
        squares_kernel,
        in_specs=[smem, smem, vmem],
        out_specs=[vmem] * 2,
        out_shape=[jax.ShapeDtypeStruct((devices, LANES), f32), jax.ShapeDtypeStruct((8, LANES), f32)],
        compiler_params=pltpu.CompilerParams(vmem_limit_bytes=2 << 20),
    )(max_norm, step_count, gradient)
    sums = lax.all_to_all(own, AXES, 0, 0, tiled=True)

    half = jax.ShapeDtypeStruct((rows // 2, cols + LANES), jnp.bfloat16)
    new_master, new_first, new_second, top, low, first = pl.pallas_call(
        adam_kernel,
        in_specs=[vmem] * 6,
        out_specs=[vmem] * 6,
        out_shape=[state] * 3 + [half] * 3,
        compiler_params=pltpu.CompilerParams(vmem_limit_bytes=54600 << 10),
    )(sums, known, master, gradient, first_moment, second_moment)

    pieces = gather_pieces(redistribute(top, low, first))
    groups = rows * RING**3 // 2 // 8
    outs = ()
    for bits in ((0, 1, 2, 3), (4, 5, 6), (7,)):
        which = [(c, b) for b in bits for c in range(3)]
        outs = pl.pallas_call(
            functools.partial(place_kernel, which),
            in_specs=[anywhere] * (len(which) + len(outs)),
            out_specs=[anywhere] * 2,
            out_shape=[
                jax.ShapeDtypeStruct((groups, 8, 2 * cols), jnp.bfloat16),
                jax.ShapeDtypeStruct((groups, 8, LANES), jnp.bfloat16),
            ],
            input_output_aliases={len(which) + i: i for i in range(len(outs))},
            scratch_shapes=[pltpu.SemaphoreType.DMA],
            compiler_params=pltpu.CompilerParams(vmem_limit_bytes=1 << 20),
        )(*[pieces[c][b] for c, b in which], *outs)
    codes, scales = outs
    return (
        new_master,
        new_first,
        new_second,
        codes.reshape(groups * 8, 2 * cols),
        scales.reshape(groups * 8, LANES),
    )


def solution(mesh):
    finer = Mesh(mesh.devices.reshape(2, RING, RING, RING), AXES)
    state = P(SHARD, "pair")
    return jax.shard_map(
        per_device,
        mesh=finer,
        in_specs=(state, state, state, state, P(), P()),
        out_specs=(state, state, state, P("pair", None), P("pair", None)),
        check_vma=False,
    )
```

```python
import functools
import math

import jax
import jax.numpy as jnp
import numpy as np
from jax import lax
from jax.experimental import pallas as pl
from jax.experimental.pallas import tpu as pltpu
from jax.sharding import Mesh
from jax.sharding import PartitionSpec as P


BLOCK = 32
LANES = 128
AXES = ("pair", "shard_0", "shard_1", "shard_2")
SHARD = ("shard_0", "shard_1", "shard_2")
RING = 4

beta_first = 0.9
beta_second = 0.99
learn_rate = 0.01
decay_rate = 0.1
adam_eps = 1e-06
scale_floor = 0.25
log_first = math.log(float(np.float32(beta_first)))
log_second = math.log(float(np.float32(beta_second)))


def everyone():
    for p in range(2):
        for z in range(RING):
            for y in range(RING):
                for x in range(RING):
                    yield p, z, y, x


def flat(p, z, y, x):
    return ((p * RING + z) * RING + y) * RING + x


def near_mask(p):
    return 1 if p == 0 else 3


def far_mask(p):
    return 3 if p == 0 else 1


def squares_kernel(
    gradient_ref, sums_ref
):
    rows, cols = gradient_ref.shape
    total = jnp.zeros((rows, LANES), jnp.float32)
    for at in range(0, cols, LANES):
        part = gradient_ref[:, at : at + LANES]
        total = total + part * part
    line = jnp.sum(total, axis=0, keepdims=True)
    sums_ref[...] = jnp.broadcast_to(line, sums_ref.shape)


def adam_kernel(
    max_norm_ref, step_ref, sums_ref, master_ref, gradient_ref, first_ref, second_ref,
    new_master_ref, new_first_ref, new_second_ref, top_ref, low_ref, one_ref,
):
    rows, cols = master_ref.shape
    line = jnp.sum(sums_ref[...], axis=0, keepdims=True)
    squares = jnp.sum(line, axis=1, keepdims=True)
    norm_limit = jnp.full((1, LANES), max_norm_ref[0], jnp.float32)
    counted = jnp.full((1, LANES), step_ref[0].astype(jnp.float32))
    clip_factor = norm_limit / jnp.maximum(jnp.sqrt(squares), norm_limit)
    first_fix = 1.0 / (1.0 - jnp.exp(counted * log_first))
    second_fix = 1.0 / (1.0 - jnp.exp(counted * log_second))

    lane = lax.broadcasted_iota(jnp.int32, (rows, LANES), 1)
    last_of_block = lane % BLOCK == BLOCK - 1
    per = LANES // BLOCK
    at_row = lax.broadcasted_iota(jnp.int32, (LANES, 2 * LANES), 0)
    at_col = lax.broadcasted_iota(jnp.int32, (LANES, 2 * LANES), 1)
    spread = at_row == (at_col // BLOCK) * BLOCK + BLOCK - 1
    gathered = at_row == (at_col % per) * BLOCK + BLOCK - 1
    picks = jnp.where(
        jnp.where(at_col < LANES, spread.astype(jnp.int32), gathered.astype(jnp.int32)) == 1, 1.0, 0.0
    ).astype(jnp.bfloat16)
    group = lane // per - (cols // LANES) * lax.axis_index("pair")

    home = lax.axis_index("pair") == lax.axis_index("shard_0") // 2

    def store(at, values):
        top, low = values[: rows // 2], values[rows // 2 :]
        top_ref[:, at] = top.astype(jnp.bfloat16)
        low_ref[:, at] = low.astype(jnp.bfloat16)
        one_ref[:, at] = jnp.where(home, low, top).astype(jnp.bfloat16)

    scales = jnp.zeros((rows, LANES), jnp.float32)
    for k in range(cols // LANES):
        at = slice(k * LANES, (k + 1) * LANES)
        master = master_ref[:, at]
        clipped = clip_factor * gradient_ref[:, at]
        new_first = beta_first * first_ref[:, at] + (1.0 - beta_first) * clipped
        new_second = beta_second * second_ref[:, at] + (1.0 - beta_second) * clipped * clipped
        update = new_first * first_fix / (jnp.sqrt(new_second * second_fix) + adam_eps) + decay_rate * master
        new_master = master - learn_rate * update
        new_master_ref[:, at] = new_master
        new_first_ref[:, at] = new_first
        new_second_ref[:, at] = new_second
        largest = jnp.abs(new_master)
        for shift in (1, 2, 4, 8, 16):
            largest = jnp.maximum(largest, pltpu.roll(largest, shift, 1))
        kept = jnp.where(last_of_block, jnp.maximum(largest, scale_floor), 0.0).astype(jnp.bfloat16)
        both = jnp.dot(kept, picks, preferred_element_type=jnp.float32)
        store(at, new_master / both[:, :LANES])
        scales = jnp.where(group == k, both[:, LANES:], scales)
    store(slice(cols, cols + LANES), scales)


def join_kernel(top_ref, one_ref, two_ref, out_ref):
    p = lax.axis_index("pair")
    home = lax.axis_index("shard_0") // 2
    cols = top_ref.shape[1] - LANES

    def fill(left, right):
        out_ref[:, :cols] = left[:, :cols]
        out_ref[:, cols : 2 * cols] = right[:, :cols]
        out_ref[:, 2 * cols :] = left[:, cols:] + right[:, cols:]

    pl.when((p == 0) & (home == 0))(lambda: fill(top_ref, one_ref))
    pl.when((p == 1) & (home == 1))(lambda: fill(one_ref, top_ref))
    pl.when((p == 0) & (home == 1))(lambda: fill(one_ref, two_ref))
    pl.when((p == 1) & (home == 0))(lambda: fill(two_ref, one_ref))


def place_kernel(which, *refs):
    pieces, (codes_ref, scales_ref, sem) = refs[: len(which)], refs[-3:]
    p, z, y, x = (lax.axis_index(a) for a in AXES)
    near = 1 + 2 * p
    far = 3 - 2 * p
    wide = codes_ref.shape[-1]
    copies = []
    for piece, (colour, bits) in zip(pieces, which):
        hop = {SHARD[(colour + i) % 3]: (bits >> i) & 1 for i in range(3)}
        for j in range(8):
            zz = z ^ (far * hop[SHARD[0]]) ^ (near * (j & 1))
            yy = y ^ (far * hop[SHARD[1]]) ^ (near * ((j >> 1) & 1))
            xx = x ^ (far * hop[SHARD[2]]) ^ (near * ((j >> 2) & 1))
            away = (zz >> 1) ^ p
            owner = zz ^ (3 * away)
            row = ((owner & 1) * (RING * RING) + yy * RING + xx) * 6 + 3 * away + colour
            copies.append(pltpu.make_async_copy(piece.at[j, :, pl.ds(0, wide)], codes_ref.at[row], sem))
            copies.append(pltpu.make_async_copy(piece.at[j, :, pl.ds(wide, LANES)], scales_ref.at[row], sem))
    for copy in copies:
        copy.start()
    for copy in copies:
        copy.wait()


def permute(value, pairs):
    return lax.ppermute(value, AXES, pairs)


def redistribute(top, low, first):
    one, two = [], []
    for q, z, y, x in everyone():
        if q == z // 2:
            one.append((flat(q, z, y, x), flat(q, 3 - z, y, x)))
        else:
            one.append((flat(q, z, y, x), flat(1 - q, z, y, x)))
            two.append((flat(q, z, y, x), flat(1 - q, 3 - z, y, x)))
    got_two = permute(low, two)
    got_one = permute(first, one)
    rows, width = top.shape
    vmem = pl.BlockSpec(memory_space=pltpu.VMEM)
    return pl.pallas_call(
        join_kernel,
        in_specs=[vmem] * 3,
        out_specs=vmem,
        out_shape=jax.ShapeDtypeStruct((rows, 2 * width - LANES), top.dtype),
        compiler_params=pltpu.CompilerParams(vmem_limit_bytes=2 << 20),
    )(top, got_one, got_two)


def gather_pieces(block):
    rows, _ = block.shape
    blocks = [block]
    for j in range(1, 8):
        pairs = []
        for q, z, y, x in everyone():
            m = near_mask(q)
            pairs.append((flat(q, z, y, x), flat(q, z ^ (m * (j & 1)), y ^ (m * ((j >> 1) & 1)), x ^ (m * (j >> 2)))))
        blocks.append(permute(block, pairs))
    whole = jnp.stack(blocks)
    third = rows // 3

    def swap(value, axis):
        pairs = []
        for q, z, y, x in everyone():
            n = [far_mask(q) if axis == i else 0 for i in range(3)]
            pairs.append((flat(q, z, y, x), flat(q, z ^ n[0], y ^ n[1], x ^ n[2])))
        return permute(value, pairs)

    pieces = [[whole[:, third * c : third * (c + 1)]] for c in range(3)]
    for step in range(3):
        count = len(pieces[0])
        for i in range(count):
            for c in range(3):
                pieces[c].append(swap(pieces[c][i], (c + step) % 3))
    return pieces


def per_device(master, gradient, first_moment, second_moment, max_norm, step_count):
    rows, cols = master.shape
    devices = 2 * RING**3
    f32 = jnp.float32
    state = jax.ShapeDtypeStruct((rows, cols), f32)
    vmem = pl.BlockSpec(memory_space=pltpu.VMEM)
    smem = pl.BlockSpec(memory_space=pltpu.SMEM)
    anywhere = pl.BlockSpec(memory_space=pl.ANY)
    own = pl.pallas_call(
        squares_kernel,
        in_specs=[vmem],
        out_specs=vmem,
        out_shape=jax.ShapeDtypeStruct((devices, LANES), f32),
        compiler_params=pltpu.CompilerParams(vmem_limit_bytes=54900 << 10),
    )(gradient)
    sums = lax.all_to_all(own, AXES, 0, 0, tiled=True)

    half = jax.ShapeDtypeStruct((rows // 2, cols + LANES), jnp.bfloat16)
    new_master, new_first, new_second, top, low, first = pl.pallas_call(
        adam_kernel,
        in_specs=[smem, smem] + [vmem] * 5,
        out_specs=[vmem] * 6,
        out_shape=[state] * 3 + [half] * 3,
        compiler_params=pltpu.CompilerParams(vmem_limit_bytes=54600 << 10),
    )(max_norm, step_count, sums, master, gradient, first_moment, second_moment)

    pieces = gather_pieces(redistribute(top, low, first))
    groups = rows * RING**3 // 2 // 8
    outs = ()
    for bits in ((0, 1, 2, 3), (4, 5, 6), (7,)):
        which = [(c, b) for b in bits for c in range(3)]
        outs = pl.pallas_call(
            functools.partial(place_kernel, which),
            in_specs=[anywhere] * (len(which) + len(outs)),
            out_specs=[anywhere] * 2,
            out_shape=[
                jax.ShapeDtypeStruct((groups, 8, 2 * cols), jnp.bfloat16),
                jax.ShapeDtypeStruct((groups, 8, LANES), jnp.bfloat16),
            ],
            input_output_aliases={len(which) + i: i for i in range(len(outs))},
            scratch_shapes=[pltpu.SemaphoreType.DMA],
            compiler_params=pltpu.CompilerParams(vmem_limit_bytes=1 << 20),
        )(*[pieces[c][b] for c, b in which], *outs)
    codes, scales = outs
    return (
        new_master,
        new_first,
        new_second,
        codes.reshape(groups * 8, 2 * cols),
        scales.reshape(groups * 8, LANES),
    )


def solution(mesh):
    finer = Mesh(mesh.devices.reshape(2, RING, RING, RING), AXES)
    state = P(SHARD, "pair")
    return jax.shard_map(
        per_device,
        mesh=finer,
        in_specs=(state, state, state, state, P(), P()),
        out_specs=(state, state, state, P("pair", None), P("pair", None)),
        check_vma=False,
    )
```

```python
import functools
import math

import jax
import jax.numpy as jnp
import numpy as np
from jax import lax
from jax.experimental import pallas as pl
from jax.experimental.pallas import tpu as pltpu
from jax.sharding import Mesh
from jax.sharding import PartitionSpec as P


BLOCK = 32
LANES = 128
AXES = ("pair", "shard_0", "shard_1", "shard_2")
SHARD = ("shard_0", "shard_1", "shard_2")
RING = 4

beta_first = 0.9
beta_second = 0.99
learn_rate = 0.01
decay_rate = 0.1
adam_eps = 1e-06
scale_floor = 0.25
log_first = math.log(float(np.float32(beta_first)))
log_second = math.log(float(np.float32(beta_second)))


def everyone():
    for p in range(2):
        for z in range(RING):
            for y in range(RING):
                for x in range(RING):
                    yield p, z, y, x


def flat(p, z, y, x):
    return ((p * RING + z) * RING + y) * RING + x


def near_mask(p):
    return 1 if p == 0 else 3


def far_mask(p):
    return 3 if p == 0 else 1


def squares_kernel(
    gradient_ref, sums_ref
):
    rows, cols = gradient_ref.shape
    total = jnp.zeros((rows, LANES), jnp.float32)
    for at in range(0, cols, LANES):
        part = gradient_ref[:, at : at + LANES]
        total = total + part * part
    line = jnp.sum(total, axis=0, keepdims=True)
    sums_ref[...] = jnp.broadcast_to(line, sums_ref.shape)


def adam_kernel(
    max_norm_ref, step_ref, sums_ref, master_ref, gradient_ref, first_ref, second_ref,
    new_master_ref, new_first_ref, new_second_ref, top_ref, low_ref, one_ref,
):
    rows, cols = master_ref.shape
    line = jnp.sum(sums_ref[...], axis=0, keepdims=True)
    squares = jnp.sum(line, axis=1, keepdims=True)
    norm_limit = jnp.full((1, LANES), max_norm_ref[0], jnp.float32)
    counted = jnp.full((1, LANES), step_ref[0].astype(jnp.float32))
    clip_factor = norm_limit / jnp.maximum(jnp.sqrt(squares), norm_limit)
    first_fix = 1.0 / (1.0 - jnp.exp(counted * log_first))
    second_fix = 1.0 / (1.0 - jnp.exp(counted * log_second))

    lane = lax.broadcasted_iota(jnp.int32, (rows, LANES), 1)
    last_of_block = lane % BLOCK == BLOCK - 1
    per = LANES // BLOCK
    at_row = lax.broadcasted_iota(jnp.int32, (LANES, 2 * LANES), 0)
    at_col = lax.broadcasted_iota(jnp.int32, (LANES, 2 * LANES), 1)
    spread = at_row == (at_col // BLOCK) * BLOCK + BLOCK - 1
    gathered = at_row == (at_col % per) * BLOCK + BLOCK - 1
    picks = jnp.where(
        jnp.where(at_col < LANES, spread.astype(jnp.int32), gathered.astype(jnp.int32)) == 1, 1.0, 0.0
    ).astype(jnp.bfloat16)
    group = lane // per - (cols // LANES) * lax.axis_index("pair")

    home = lax.axis_index("pair") == lax.axis_index("shard_0") // 2

    def store(at, values):
        top, low = values[: rows // 2], values[rows // 2 :]
        top_ref[:, at] = top.astype(jnp.bfloat16)
        low_ref[:, at] = low.astype(jnp.bfloat16)
        one_ref[:, at] = jnp.where(home, low, top).astype(jnp.bfloat16)

    scales = jnp.zeros((rows, LANES), jnp.float32)
    for k in range(cols // LANES):
        at = slice(k * LANES, (k + 1) * LANES)
        master = master_ref[:, at]
        clipped = clip_factor * gradient_ref[:, at]
        new_first = beta_first * first_ref[:, at] + (1.0 - beta_first) * clipped
        new_second = beta_second * second_ref[:, at] + (1.0 - beta_second) * clipped * clipped
        update = new_first * first_fix / (jnp.sqrt(new_second * second_fix) + adam_eps) + decay_rate * master
        new_master = master - learn_rate * update
        new_master_ref[:, at] = new_master
        new_first_ref[:, at] = new_first
        new_second_ref[:, at] = new_second
        largest = jnp.abs(new_master)
        for shift in (1, 2, 4, 8, 16):
            largest = jnp.maximum(largest, pltpu.roll(largest, shift, 1))
        kept = jnp.where(last_of_block, jnp.maximum(largest, scale_floor), 0.0).astype(jnp.bfloat16)
        both = jnp.dot(kept, picks, preferred_element_type=jnp.float32)
        store(at, new_master / both[:, :LANES])
        scales = jnp.where(group == k, both[:, LANES:], scales)
    store(slice(cols, cols + LANES), scales)


def join_kernel(top_ref, one_ref, two_ref, out_ref):
    p = lax.axis_index("pair")
    home = lax.axis_index("shard_0") // 2
    cols = top_ref.shape[1] - LANES

    def fill(left, right):
        out_ref[:, :cols] = left[:, :cols]
        out_ref[:, cols : 2 * cols] = right[:, :cols]
        out_ref[:, 2 * cols :] = left[:, cols:] + right[:, cols:]

    pl.when((p == 0) & (home == 0))(lambda: fill(top_ref, one_ref))
    pl.when((p == 1) & (home == 1))(lambda: fill(one_ref, top_ref))
    pl.when((p == 0) & (home == 1))(lambda: fill(one_ref, two_ref))
    pl.when((p == 1) & (home == 0))(lambda: fill(two_ref, one_ref))


def place_kernel(which, *refs):
    pieces, (codes_ref, scales_ref, sem) = refs[: len(which)], refs[-3:]
    p, z, y, x = (lax.axis_index(a) for a in AXES)
    near = 1 + 2 * p
    far = 3 - 2 * p
    wide = codes_ref.shape[-1]
    copies = []
    for piece, (colour, bits) in zip(pieces, which):
        hop = {SHARD[(colour + i) % 3]: (bits >> i) & 1 for i in range(3)}
        for j in range(8):
            zz = z ^ (3 * hop[SHARD[0]]) ^ (j & 1)
            yy = y ^ (far * hop[SHARD[1]]) ^ (near * ((j >> 1) & 1))
            xx = x ^ (far * hop[SHARD[2]]) ^ (near * ((j >> 2) & 1))
            away = (zz >> 1) ^ p
            owner = zz ^ (3 * away)
            row = ((owner & 1) * (RING * RING) + yy * RING + xx) * 6 + 3 * away + colour
            copies.append(pltpu.make_async_copy(piece.at[j, :, pl.ds(0, wide)], codes_ref.at[row], sem))
            copies.append(pltpu.make_async_copy(piece.at[j, :, pl.ds(wide, LANES)], scales_ref.at[row], sem))
    for copy in copies:
        copy.start()
    for copy in copies:
        copy.wait()


def permute(value, pairs):
    return lax.ppermute(value, AXES, pairs)


def redistribute(top, low, first):
    one, two = [], []
    for q, z, y, x in everyone():
        if q == z // 2:
            one.append((flat(q, z, y, x), flat(q, 3 - z, y, x)))
        else:
            one.append((flat(q, z, y, x), flat(1 - q, z, y, x)))
            two.append((flat(q, z, y, x), flat(1 - q, 3 - z, y, x)))
    got_two = permute(low, two)
    got_one = permute(first, one)
    rows, width = top.shape
    vmem = pl.BlockSpec(memory_space=pltpu.VMEM)
    return pl.pallas_call(
        join_kernel,
        in_specs=[vmem] * 3,
        out_specs=vmem,
        out_shape=jax.ShapeDtypeStruct((rows, 2 * width - LANES), top.dtype),
        compiler_params=pltpu.CompilerParams(vmem_limit_bytes=2 << 20),
    )(top, got_one, got_two)


def gather_pieces(block):
    rows, _ = block.shape
    blocks = [block]
    for j in range(1, 8):
        pairs = []
        for q, z, y, x in everyone():
            m = near_mask(q)
            pairs.append((flat(q, z, y, x), flat(q, z ^ (j & 1), y ^ (m * ((j >> 1) & 1)), x ^ (m * (j >> 2)))))
        blocks.append(permute(block, pairs))
    whole = jnp.stack(blocks)
    third = rows // 3

    def swap(value, axis):
        pairs = []
        for q, z, y, x in everyone():
            n = [(3 if i == 0 else far_mask(q)) if axis == i else 0 for i in range(3)]
            pairs.append((flat(q, z, y, x), flat(q, z ^ n[0], y ^ n[1], x ^ n[2])))
        return permute(value, pairs)

    pieces = [[whole[:, third * c : third * (c + 1)]] for c in range(3)]
    for step in range(3):
        count = len(pieces[0])
        for i in range(count):
            for c in range(3):
                pieces[c].append(swap(pieces[c][i], (c + step) % 3))
    return pieces


def per_device(master, gradient, first_moment, second_moment, max_norm, step_count):
    rows, cols = master.shape
    devices = 2 * RING**3
    f32 = jnp.float32
    state = jax.ShapeDtypeStruct((rows, cols), f32)
    vmem = pl.BlockSpec(memory_space=pltpu.VMEM)
    smem = pl.BlockSpec(memory_space=pltpu.SMEM)
    anywhere = pl.BlockSpec(memory_space=pl.ANY)
    own = pl.pallas_call(
        squares_kernel,
        in_specs=[vmem],
        out_specs=vmem,
        out_shape=jax.ShapeDtypeStruct((devices, LANES), f32),
        compiler_params=pltpu.CompilerParams(vmem_limit_bytes=54900 << 10),
    )(gradient)
    sums = lax.all_to_all(own, AXES, 0, 0, tiled=True)

    half = jax.ShapeDtypeStruct((rows // 2, cols + LANES), jnp.bfloat16)
    new_master, new_first, new_second, top, low, first = pl.pallas_call(
        adam_kernel,
        in_specs=[smem, smem] + [vmem] * 5,
        out_specs=[vmem] * 6,
        out_shape=[state] * 3 + [half] * 3,
        compiler_params=pltpu.CompilerParams(vmem_limit_bytes=54600 << 10),
    )(max_norm, step_count, sums, master, gradient, first_moment, second_moment)

    pieces = gather_pieces(redistribute(top, low, first))
    groups = rows * RING**3 // 2 // 8
    outs = ()
    for bits in ((0, 1, 2, 3), (4, 5, 6), (7,)):
        which = [(c, b) for b in bits for c in range(3)]
        outs = pl.pallas_call(
            functools.partial(place_kernel, which),
            in_specs=[anywhere] * (len(which) + len(outs)),
            out_specs=[anywhere] * 2,
            out_shape=[
                jax.ShapeDtypeStruct((groups, 8, 2 * cols), jnp.bfloat16),
                jax.ShapeDtypeStruct((groups, 8, LANES), jnp.bfloat16),
            ],
            input_output_aliases={len(which) + i: i for i in range(len(outs))},
            scratch_shapes=[pltpu.SemaphoreType.DMA],
            compiler_params=pltpu.CompilerParams(vmem_limit_bytes=1 << 20),
        )(*[pieces[c][b] for c, b in which], *outs)
    codes, scales = outs
    return (
        new_master,
        new_first,
        new_second,
        codes.reshape(groups * 8, 2 * cols),
        scales.reshape(groups * 8, LANES),
    )


def solution(mesh):
    finer = Mesh(mesh.devices.reshape(2, RING, RING, RING), AXES)
    state = P(SHARD, "pair")
    return jax.shard_map(
        per_device,
        mesh=finer,
        in_specs=(state, state, state, state, P(), P()),
        out_specs=(state, state, state, P("pair", None), P("pair", None)),
        check_vma=False,
    )
```
